32 devices in a mesh: op: 8 (over y, x, core), tm: 4 (over z).
Axes of the slice: x: 2, y: 2, z: 4, core: 2. Of those that a mesh axis runs over, the one named last changes fastest.
Arguments:
- phi: bfloat16 [256, 32, 2, 128, 128], P('op', 'tm'), may hold values from -6 to 6
- tau_fwd: bfloat16 [2, 32, 2, 128, 128], P(None, 'tm'), may hold values from -0.375 to 0.375
- tau_bwd: bfloat16 [2, 32, 2, 128, 128], P(None, 'tm'), may hold values from -0.375 to 0.375
- src_times: int32 [2], replicated, may hold values from 0 to 31
- partner: int32 [256], replicated, may hold values from 0 to 255, each once
Outputs:
- corr: float32 [256, 2, 32, 2, 256], P('op', None, 'tm')
The draws below stay inside these ranges and needn't reach their ends.
Inputs may be any that keep to these rules, and one draw needn't show every extreme that they name: partner is a permutation of the operators. `src_times`: source times may repeat.
All inputs are finite; a program needn't handle non-finite values.
Results may differ from the reference program's by a relative error of at most 0.0041.
Values may be sent and summed in bfloat16 or wider, within the bound.
No kernel may reach another device: no remote copies, remote signals or barrier semaphores. Data moves between devices by JAX's collectives and lax.ppermute only.
A program may use at most 256 MiB of HBM per device.

```python
import jax
import jax.numpy as jnp
from jax import lax

NV = 128
OPS = 256
NSRC = 2
NT = 32


def level_of(stream_key, shape, cuts, smallest, top_value):
    def one(dim, blocks):
        draws = jax.random.uniform(jax.random.fold_in(jax.random.fold_in(stream_key, 6), dim), (blocks,), jnp.float32, smallest / len(cuts), top_value / len(cuts))
        return jnp.repeat(jnp.exp(draws), shape[dim] // blocks).reshape((-1,) + (1,) * (len(shape) - dim - 1))

    gain = one(*cuts[0])
    for cut in cuts[1:]:
        gain = gain * one(*cut)
    return gain


def centred(rng, dims, scale, limit, pieces=(), kind=jnp.bfloat16):
    loudness = level_of(rng, dims, pieces, -0.22, 0.18) if pieces else 1.0
    values = jax.random.normal(rng, dims, jnp.float32) * scale * loudness
    return jnp.minimum(jnp.maximum(values, -limit), limit).astype(kind)


def setup_inputs(seed: int = 0) -> dict:
    keys = jax.random.split(jax.random.key(seed), 6)
    return {
        "phi": centred(keys[0], (OPS, NT, 2, NV, NV), 1.0, 6.0, ((0, 8), (1, 4))),
        "tau_fwd": centred(keys[1], (NSRC, NT, 2, NV, NV), (2 * NV) ** -0.5, 0.375, ((1, 4),)),
        "tau_bwd": centred(keys[2], (NSRC, NT, 2, NV, NV), (2 * NV) ** -0.5, 0.375, ((1, 4),)),
        "src_times": jax.random.randint(keys[3], (NSRC,), 0, NT).astype(jnp.int32),
        "partner": jax.random.permutation(keys[4], OPS).astype(jnp.int32),
    }


def rounded(value):
    low = lax.optimization_barrier(value.astype(jnp.bfloat16))
    return low.astype(jnp.float32)


def complex_product(spec, left_re, left_im, right_re, right_im):
    def inner(first, second):
        return jnp.einsum(spec, first, second)
    return inner(left_re, right_re) - inner(left_im, right_im), inner(left_re, right_im) + inner(left_im, right_re)


def reference(phi, tau_fwd, tau_bwd, src_times, partner):
    source = jnp.take(phi, src_times.astype(jnp.int32), axis=1).astype(jnp.float32)
    source_re = source[:, :, 0]
    source_im = source[:, :, 1]

    def one_time(when):
        fields = lax.dynamic_index_in_dim(phi, when, 1, False).astype(jnp.float32)
        fwd = lax.dynamic_index_in_dim(tau_fwd, when, 1, False).astype(jnp.float32)
        bwd = lax.dynamic_index_in_dim(tau_bwd, when, 1, False).astype(jnp.float32)
        left_re, left_im = complex_product("sab,jbc->jsac", fwd[:, 0], fwd[:, 1], fields[:, 0], fields[:, 1])
        left_re, left_im = rounded(left_re), rounded(left_im)
        sink_re, sink_im = complex_product("jsac,scd->jsad", left_re, left_im, bwd[:, 0], bwd[:, 1])
        sink_re, sink_im = rounded(sink_re), rounded(sink_im)
        real_part = jnp.einsum("jsad,ksad->jsk", sink_re, source_re) + jnp.einsum("jsad,ksad->jsk", sink_im, source_im)
        imag_part = jnp.einsum("jsad,ksad->jsk", sink_im, source_re) - jnp.einsum("jsad,ksad->jsk", sink_re, source_im)
        return jnp.stack([real_part, imag_part], 2) / NV

    result = lax.map(one_time, jnp.arange(NT, dtype=jnp.int32))
    result = jnp.transpose(result, (1, 2, 0, 3, 4))
    return jnp.take(result, partner.astype(jnp.int32), axis=4)
```

```python
import jax
import jax.numpy as jnp
from jax import lax
from jax.sharding import PartitionSpec as P


def joined(top, low):
    return jnp.concatenate(
        [jnp.concatenate(top, 3), jnp.concatenate(low, 3)], 2
    )


def body(phi, tau_fwd, tau_bwd, src_times, partner):
    ops, time_local = phi.shape[:2]
    sources = tau_fwd.shape[0]
    width = phi.shape[-1]
    here = lax.axis_index("tm")

    fields = []
    for source_index in range(sources):
        when = src_times[source_index]
        local = lax.dynamic_index_in_dim(phi, when % time_local, 1, False)
        fields.append(jnp.where(here == when // time_local, local, 0).astype(phi.dtype))
    own = jnp.stack(fields, 0).transpose(0, 3, 1, 2, 4).reshape(sources * width, ops, 2 * width)
    piece = lax.psum_scatter(own, "tm", scatter_dimension=0, tiled=True)

    left = joined(
        [tau_fwd[:, :, 0], -tau_fwd[:, :, 1]], [tau_fwd[:, :, 1], tau_fwd[:, :, 0]]
    )
    stacked = phi.reshape(ops, time_local, 2 * width, width)
    a = jnp.einsum("stxb,jtbc->stjxc", left, stacked, preferred_element_type=jnp.float32)
    a = a.astype(jnp.bfloat16)
    piece, a = lax.optimization_barrier((piece, a))
    whole = lax.all_gather(piece, ("op", "tm"), axis=0, tiled=True)
    gathered = whole.reshape(-1, sources, width, ops, 2 * width)
    groups = gathered.shape[0]

    a = a.reshape(sources, time_local, ops, 2, width, width)
    a = jnp.concatenate([a[:, :, :, 0], a[:, :, :, 1]], 4)
    back_re, back_im = tau_bwd[:, :, 0], tau_bwd[:, :, 1]
    parts = []
    for right in (
        joined([back_re, back_im], [-back_im, back_re]),
        joined([back_im, -back_re], [back_re, back_im]),
    ):
        p = jnp.einsum("stjac,stcd->stjad", a, right, preferred_element_type=jnp.float32)
        p = p.astype(jnp.bfloat16)
        q = jnp.einsum("stjad,gsakd->jstgk", p, gathered, preferred_element_type=jnp.float32)
        parts.append(q.reshape(ops, sources, time_local, groups * ops))
    q = jnp.stack(parts, 3) / width
    return jnp.take(q, partner, axis=4, mode="clip", unique_indices=True)


def solution(mesh):
    in_specs = (
        P("op", "tm", None, None, None),
        P(None, "tm", None, None, None),
        P(None, "tm", None, None, None),
        P(),
        P(),
    )
    out_specs = P("op", None, "tm", None, None)
    return jax.shard_map(body, mesh=mesh, in_specs=in_specs, out_specs=out_specs, check_vma=False)
```
